32 devices in a mesh: task: 4 (over y, core), param: 8 (over z, x).
Axes of the slice: x: 2, y: 2, z: 4, core: 2. Of those that a mesh axis runs over, the one named last changes fastest.
Arguments:
- params: bfloat16 [16, 512, 4096], P('task', 'param'), may hold values from -6 to 6
- fisher: float32 [16, 512, 4096], P('task', 'param'), may hold values from 3e-06 to 1, as said below
Outputs:
- merged: bfloat16 [512, 4096], P('param')
The draws below stay inside these ranges and needn't reach their ends.
Inputs may be any that keep to these rules, and one draw needn't show every extreme that they name: `fisher`: every entry is positive; scales differ strongly between tasks and between regions of rows.
All inputs are finite; a program needn't handle non-finite values.
Results may differ from the reference program's by a relative error of at most 0.00045.
Values may be sent and summed in bfloat16 or wider, within the bound.
A program may use at most 64 MiB of HBM per device.

```python
import math
import jax
import jax.numpy as jnp
from jax import lax

FF = 4096
TASKS = 16
ROWS = 512


def draw_fisher(key, part):
    first, second, third = jax.random.split(key, 3)
    region = jnp.exp(jax.random.uniform(first, (TASKS, 8), jnp.float32, math.log(1.0 / 256.0), 0.0))
    region = jnp.repeat(region, ROWS // 8, axis=1)
    base = jnp.exp(jax.random.uniform(second, (TASKS, ROWS, FF), jnp.float32, math.log(0.001), 0.0))
    return (base * region[:, :, None]).astype(jnp.float32)


def block_levels(own_key, dims, cuts, least, top_value):
    gain, own = 1.0, jax.random.fold_in(own_key, 6)
    for position, blocks in cuts:
        draws = jnp.exp(jax.random.uniform(jax.random.fold_in(own, position), (blocks,), jnp.float32, least / len(cuts), top_value / len(cuts)))
        gain = gain * jnp.repeat(draws, dims[position] // blocks).reshape([-1 if axis == position else 1 for axis in range(len(dims))])
    return gain


def scatter_about(own_key, dims, spread, bound, shards=(), kind=jnp.bfloat16):
    factor_of = block_levels(own_key, dims, shards, -0.22, 0.18) if shards else 1.0
    values = jax.random.normal(own_key, dims, jnp.float32) * spread * factor_of
    return jnp.minimum(jnp.maximum(values, -bound), bound).astype(kind)


def setup_inputs(seed: int = 0) -> dict:
    arg_keys = jax.random.split(jax.random.key(seed), 3)
    return {
        "params": scatter_about(arg_keys[0], (TASKS, ROWS, FF), 1.0, 6.0, ((0, 4), (1, 8))),
        "fisher": draw_fisher(jax.random.fold_in(arg_keys[2], 71), 0),
    }


def reference(params, fisher):
    peak = jnp.max(fisher, axis=(1, 2))
    total = jnp.sum(fisher, axis=(1, 2))
    count = float(ROWS * FF)
    factor = count * peak / total

    def one_task(carry, items):
        theta, info, top, mult = items
        weight = jnp.clip(info / top, 0.002, 0.25) * mult
        return (carry[0] + weight * theta.astype(jnp.float32), carry[1] + weight), None

    start = (jnp.zeros((ROWS, FF), jnp.float32), jnp.zeros((ROWS, FF), jnp.float32))
    sums, unused = lax.scan(one_task, start, (params, fisher, peak, factor))
    return (sums[0] / sums[1]).astype(jnp.bfloat16)
```

```python
import functools

import jax
import jax.numpy as jnp
from jax import lax
from jax.experimental import pallas as pl
from jax.experimental.pallas import tpu as pltpu
from jax.sharding import PartitionSpec as P

MESH = pl.DeviceIdType.MESH
LANES = 128
SPAN = 126.0
HEAD = 8


def encode(value):
    size = jnp.exp2(jnp.abs(value) * (2.0 * SPAN) - SPAN)
    return jnp.where(value < 0, -size, size).astype(jnp.bfloat16)


def decode(code):
    code = code.astype(jnp.float32)
    size = (jnp.log2(jnp.abs(code)) + SPAN) * (0.5 / SPAN)
    return jnp.where(code < 0, -size, size)


def kernel(tasks, groups, params_hbm, fisher_hbm, out, fisher, params, fisher_in, params_in, mine, stats, sent, landed,
           kept, load_f, load_p, push_f, push_p, in_f, in_p, stat_send, stat_recv, y_send, y_recv, res_send, res_recv,
           near_send, near_recv):
    count, rows, width = fisher.shape
    chips = tasks // 2
    half, piece = width // 2, width // tasks
    chunks = piece // LANES
    task, param = lax.axis_index("task"), lax.axis_index("param")
    chip, core = task // 2, task % 2
    f32 = jnp.float32

    def device(shift, other_core, member):
        to = lax.rem(chip + shift, chips) * 2 + (1 - core if other_core else core)
        return {"task": to, "param": lax.rem(param + member, groups)}

    partner = device(0, True, 0)

    loads_f = [
        [pltpu.make_async_copy(fisher_hbm.at[t, :, pl.ds(h * half, half)], fisher.at[t, :, pl.ds(h * half, half)],
                               load_f.at[t, h]) for h in range(2)] for t in range(count)]
    own = pl.ds(pl.multiple_of(core * half, LANES), half)
    load_params = pltpu.make_async_copy(params_hbm.at[:, :, own], params, load_p)
    for pair in loads_f:
        for copy in pair:
            copy.start()
    load_params.start()

    barrier = pltpu.get_barrier_semaphore()
    greeted = [device(0, other, s) for s in range(groups) for other in (False, True) if other or s]
    greeted += [device(s, False, 0) for s in range(1, chips)]
    for who in greeted:
        pl.semaphore_signal(barrier, inc=1, device_id=who, device_id_type=MESH)

    tops, sums = [], []
    for t in range(count):
        top = total = None
        for h in range(2):
            loads_f[t][h].wait()

            def over(step, carry, t=t, h=h):
                block = fisher[t, :, pl.ds(pl.multiple_of(h * half + step * LANES, LANES), LANES)]
                return jnp.maximum(carry[0], block), carry[1] + block

            if h == 0:
                first = fisher[t, :, 0:LANES]
                top, total = lax.fori_loop(1, half // LANES, over, (first, first), unroll=5)
            else:
                top, total = lax.fori_loop(0, half // LANES, over, (top, total), unroll=4)
        tops.append(jnp.max(top, axis=0, keepdims=True))
        sums.append(jnp.sum(total, axis=0, keepdims=True))
    top = jnp.max(jnp.concatenate(tops, axis=0), axis=1, keepdims=True)
    total = jnp.sum(jnp.concatenate(sums, axis=0), axis=1, keepdims=True)
    column = jnp.broadcast_to(jnp.concatenate([top, total], axis=0), (2 * count, LANES))
    lane = lax.broadcasted_iota(jnp.int32, (2 * count, LANES), 1)
    row = lax.broadcasted_iota(jnp.int32, (2 * count, LANES), 0)
    packed = jnp.sum(jnp.where(lane == row, column, 0.0), axis=0, keepdims=True)
    mine[...] = jnp.broadcast_to(packed, mine.shape)

    pl.semaphore_wait(barrier, len(greeted))

    stat_copies = []
    for s in range(groups - 1, -1, -1):
        for other in (0, 1):
            if not s and not other:
                continue
            stat_copies.append(pltpu.make_async_remote_copy(
                src_ref=mine.at[pl.ds(0, 1)], dst_ref=stats.at[other, pl.ds(s, 1)], send_sem=stat_send.at[other, s],
                recv_sem=stat_recv.at[other, s], device_id=device(0, bool(other), s), device_id_type=MESH))
    for copy in stat_copies:
        copy.start()
    stats[0, 0:1, :] = packed

    def place(shift, k):
        return pl.multiple_of(lax.rem(chip + shift, chips) * piece + k * LANES, LANES)

    order = [(shift, k) for shift in range(1, chips) for k in range(chunks)] + [(0, k) for k in range(chunks)]

    def push_copies(shift, k):
        there = pl.ds(pl.multiple_of((1 - core) * half + place(shift, k), LANES), LANES)
        here = pl.ds(place(shift, k), LANES)
        return [
            pltpu.make_async_remote_copy(
                src_ref=fisher_hbm.at[:, :, there], dst_ref=fisher_in.at[:, :, here], send_sem=push_f.at[shift, k],
                recv_sem=in_f.at[shift, k], device_id=partner, device_id_type=MESH),
            pltpu.make_async_remote_copy(
                src_ref=params_hbm.at[:, :, there], dst_ref=params_in.at[:, :, here], send_sem=push_p.at[shift, k],
                recv_sem=in_p.at[shift, k], device_id=partner, device_id_type=MESH)]

    for shift, k in order:
        for copy in push_copies(shift, k):
            copy.start()

    load_params.wait()
    for copy in stat_copies:
        copy.wait_recv()

    size = float(rows * groups * width)
    spread = []
    for other in (0, 1):
        peaks = jnp.max(stats[other], axis=0, keepdims=True)
        totals = jnp.sum(stats[other], axis=0, keepdims=True)
        for t in range(count):
            peak = jnp.broadcast_to(peaks[:, t:t + 1], (8, LANES))
            gain = size / jnp.broadcast_to(totals[:, count + t:count + t + 1], (8, LANES))
            factor = peak * gain
            spread.append((gain, 0.002 * factor, 0.25 * factor))

    def tall(a):
        return jnp.concatenate([a] * (rows // 8), axis=0)

    def partial(shift, k):
        at = place(shift, k)
        here = pl.ds(at, LANES)
        full = pl.ds(pl.multiple_of(core * half + at, LANES), LANES)
        for copy in push_copies(shift, k):
            copy.wait_recv()
        numer = denom = None
        for other in (0, 1):
            for t in range(count):
                gain, low, high = (tall(a) for a in spread[other * count + t])
                info = fisher_in[t, :, here] if other else fisher[t, :, full]
                theta = (params_in if other else params)[t, :, here].astype(f32)
                weight = jnp.minimum(jnp.maximum(info * gain, low), high)
                numer = weight * theta if numer is None else numer + weight * theta
                denom = weight if denom is None else denom + weight
        return numer, denom

    def y_copy(shift, k):
        return pltpu.make_async_remote_copy(
            src_ref=sent.at[shift - 1, k], dst_ref=landed.at[shift - 1, k], send_sem=y_send.at[shift - 1, k],
            recv_sem=y_recv.at[shift - 1, k], device_id=device(shift, False, 0), device_id_type=MESH)

    def columns(shift, k):
        return pl.ds(pl.multiple_of(core * half + place(shift, k), LANES), LANES)

    def res_copy(shift, k):
        where = out.at[:, columns(0, k)]
        return pltpu.make_async_remote_copy(
            src_ref=where, dst_ref=where, send_sem=res_send.at[shift - 1, k], recv_sem=res_recv.at[shift - 1, k],
            device_id=device(shift, False, 0), device_id_type=MESH)

    def near_copy(shift, k):
        where = out.at[:, columns(chips - shift if shift else 0, k)]
        return pltpu.make_async_remote_copy(
            src_ref=where, dst_ref=where, send_sem=near_send.at[shift, k], recv_sem=near_recv.at[shift, k],
            device_id=partner, device_id_type=MESH)

    head = lax.broadcasted_iota(jnp.int32, (HEAD, LANES), 0)

    for shift in range(1, chips):
        def send(k, carry, shift=shift):
            numer, denom = partial(shift, k)
            mean = numer / denom
            reach = jnp.maximum(jnp.max(jnp.abs(mean), axis=0, keepdims=True) * 1.01, 1e-35)
            reach = reach.astype(jnp.bfloat16).astype(f32)
            most = (jnp.max(denom, axis=0, keepdims=True) * 1.01).astype(jnp.bfloat16).astype(f32)
            box = sent.at[shift - 1, k]
            box[0:rows] = encode(mean * (1.0 / reach))
            box[rows:2 * rows] = encode(2.0 * jnp.sqrt(denom * (1.0 / most)) - 1.0)
            box[2 * rows:2 * rows + HEAD] = jnp.where(head == 0, reach, most).astype(jnp.bfloat16)
            y_copy(shift, k).start()
            return carry

        lax.fori_loop(0, chunks, send, 0)

    def keep(k, carry):
        kept[k, 0], kept[k, 1] = partial(0, k)
        return carry

    lax.fori_loop(0, chunks, keep, 0)

    def finish(k, carry):
        numer, denom = kept[k, 0], kept[k, 1]
        for shift in range(1, chips):
            y_copy(shift, k).wait_recv()
            box = landed.at[shift - 1, k]
            scale = box[2 * rows:2 * rows + HEAD].astype(f32)
            root = decode(box[rows:2 * rows]) * 0.5 + 0.5
            weight = root * root * scale[1:2]
            numer = numer + decode(box[0:rows]) * scale[0:1] * weight
            denom = denom + weight
        out[:, columns(0, k)] = (numer / denom).astype(out.dtype)
        for shift in range(1, chips):
            res_copy(shift, k).start()
        near_copy(0, k).start()
        return carry

    lax.fori_loop(0, chunks, finish, 0)

    for shift in range(1, chips):
        def forward(k, carry, shift=shift):
            res_copy(shift, k).wait_recv()
            near_copy(shift, k).start()
            return carry

        lax.fori_loop(0, chunks, forward, 0)

    for copy in stat_copies:
        copy.wait_send()
    for shift, k in order:
        for copy in push_copies(shift, k):
            copy.wait_send()
        if shift:
            y_copy(shift, k).wait_send()
            res_copy(shift, k).wait_send()
        near_copy(shift, k).wait()


def local(mesh, params, fisher):
    count, rows, width = fisher.shape
    tasks, groups = mesh.shape["task"], mesh.shape["param"]
    chips, piece = tasks // 2, width // tasks
    chunks = piece // LANES
    far = max(1, chips - 1)
    half = width // 2
    f32, bf16, dma = jnp.float32, jnp.bfloat16, pltpu.SemaphoreType.DMA
    return pl.pallas_call(
        functools.partial(kernel, tasks, groups),
        out_shape=pltpu.VMEM((rows, width), bf16),
        in_specs=[pl.BlockSpec(memory_space=pltpu.HBM)] * 2,
        out_specs=pl.BlockSpec(memory_space=pltpu.VMEM),
        scratch_shapes=[
            pltpu.VMEM((count, rows, width), f32),
            pltpu.VMEM((count, rows, half), bf16),
            pltpu.VMEM((count, rows, half), f32),
            pltpu.VMEM((count, rows, half), bf16),
            pltpu.VMEM((8, LANES), f32),
            pltpu.VMEM((2, groups, LANES), f32),
            pltpu.VMEM((far, chunks, 2 * rows + HEAD, LANES), bf16),
            pltpu.VMEM((far, chunks, 2 * rows + HEAD, LANES), bf16),
            pltpu.VMEM((chunks, 2, rows, LANES), f32),
            dma((count, 2)),
            dma(()),
            dma((chips, chunks)),
            dma((chips, chunks)),
            dma((chips, chunks)),
            dma((chips, chunks)),
            dma((2, groups)),
            dma((2, groups)),
            dma((far, chunks)),
            dma((far, chunks)),
            dma((far, chunks)),
            dma((far, chunks)),
            dma((chips, chunks)),
            dma((chips, chunks)),
        ],
        compiler_params=pltpu.CompilerParams(collective_id=0, has_side_effects=True),
        name="merge",
    )(params, fisher)


def solution(mesh):
    in_specs = (P("task", "param", None), P("task", "param", None))
    out_specs = P("param", None)
    return jax.shard_map(
        functools.partial(local, mesh), mesh=mesh, in_specs=in_specs, out_specs=out_specs, check_vma=False)
```

```python
import functools

import jax
import jax.numpy as jnp
from jax import lax
from jax.experimental import pallas as pl
from jax.experimental.pallas import tpu as pltpu
from jax.sharding import PartitionSpec as P

MESH = pl.DeviceIdType.MESH
LANES = 128
SPAN = 126.0
HEAD = 2


def encode(value):
    size = jnp.exp2(jnp.abs(value) * (2.0 * SPAN) - SPAN)
    return jnp.where(value < 0, -size, size).astype(jnp.bfloat16)


def decode(code):
    code = code.astype(jnp.float32)
    size = (jnp.log2(jnp.abs(code)) + SPAN) * (0.5 / SPAN)
    return jnp.where(code < 0, -size, size)


def kernel(tasks, groups, counts, params_hbm, fisher_hbm, out, fisher, params, fisher_in, params_in, mine, stats, sent,
           landed, kept, load_f, load_p, push_f, push_p, in_f, in_p, stat_send, stat_recv, y_send, y_recv, res_send,
           res_recv, near_send, near_recv):
    count, rows, width = fisher.shape
    chips = tasks // 2
    half = width // 2
    starts = (0, counts[0] * chips * LANES)
    task, param = lax.axis_index("task"), lax.axis_index("param")
    chip, core = task // 2, task % 2
    chunks = counts[0] + core * (counts[1] - counts[0])
    f32 = jnp.float32

    def device(shift, other_core, member):
        to = lax.rem(chip + shift, chips) * 2 + (1 - core if other_core else core)
        return {"task": to, "param": lax.rem(param + member, groups)}

    def remote(src, dst, send, recv, who):
        return pltpu.make_async_remote_copy(
            src_ref=src, dst_ref=dst, send_sem=send, recv_sem=recv, device_id=who, device_id_type=MESH)

    def on_each_core(act):
        for c in (0, 1):
            pl.when(core == c)(functools.partial(act, c))

    partner = device(0, True, 0)

    loads_f = [
        [pltpu.make_async_copy(fisher_hbm.at[t, :, pl.ds(h * half, half)], fisher.at[t, :, pl.ds(h * half, half)],
                               load_f.at[t, h]) for h in range(2)] for t in range(count)]
    load_params = pltpu.make_async_copy(params_hbm, params, load_p)
    for pair in loads_f:
        for copy in pair:
            copy.start()

    barrier = pltpu.get_barrier_semaphore()
    greeted = [device(0, other, s) for s in range(groups) for other in (False, True) if other or s]
    greeted += [device(s, False, 0) for s in range(1, chips)]
    for who in greeted:
        pl.semaphore_signal(barrier, inc=1, device_id=who, device_id_type=MESH)

    tops, sums = [], []
    for t in range(count):
        top = total = None
        for h in range(2):
            loads_f[t][h].wait()

            def over(step, carry, t=t, h=h):
                block = fisher[t, :, pl.ds(pl.multiple_of(h * half + step * LANES, LANES), LANES)]
                return jnp.maximum(carry[0], block), carry[1] + block

            if h == 0:
                first = fisher[t, :, 0:LANES]
                top, total = lax.fori_loop(1, half // LANES, over, (first, first), unroll=5)
            else:
                top, total = lax.fori_loop(0, half // LANES, over, (top, total), unroll=4)
        tops.append(jnp.max(top, axis=0, keepdims=True))
        sums.append(jnp.sum(total, axis=0, keepdims=True))
    load_params.start()
    top = jnp.max(jnp.concatenate(tops, axis=0), axis=1, keepdims=True)
    total = jnp.sum(jnp.concatenate(sums, axis=0), axis=1, keepdims=True)
    column = jnp.broadcast_to(jnp.concatenate([top, total], axis=0), (2 * count, LANES))
    lane = lax.broadcasted_iota(jnp.int32, (2 * count, LANES), 1)
    row = lax.broadcasted_iota(jnp.int32, (2 * count, LANES), 0)
    packed = jnp.sum(jnp.where(lane == row, column, 0.0), axis=0, keepdims=True)
    mine[...] = jnp.broadcast_to(packed, mine.shape)

    pl.semaphore_wait(barrier, len(greeted))

    for s in range(groups - 1, -1, -1):
        for other in (0, 1):
            if s or other:
                remote(mine.at[pl.ds(0, 1)], stats.at[pl.ds(other * groups + s, 1)], stat_send, stat_recv,
                       device(0, bool(other), s)).start()
    stats[0:1, :] = packed
    others = stats.at[pl.ds(1, 2 * groups - 1)]
    stat_all = remote(others, others, stat_send, stat_recv, partner)

    def block(c, shift):
        size = counts[c] * LANES
        return pl.multiple_of(lax.rem(chip + shift, chips) * size, LANES), size

    def push_copies(c, shift):
        at, size = block(c, shift)
        there = pl.ds(pl.multiple_of(starts[c] + at, LANES), size)
        here = pl.ds(at, size)
        return [remote(fisher_hbm.at[:, :, there], fisher_in.at[:, :, here], push_f, in_f.at[shift], partner),
                remote(params_hbm.at[:, :, there], params_in.at[:, :, here], push_p, in_p.at[shift], partner)]

    turns = list(range(1, chips)) + [0]

    @on_each_core
    def _(c):
        for shift in turns:
            for copy in push_copies(1 - c, shift):
                copy.start()

    load_params.wait()
    stat_all.wait_recv()

    size = float(rows * groups * width)
    spread = []
    for other in (0, 1):
        told = stats[other * groups:(other + 1) * groups]
        peaks = jnp.max(told, axis=0, keepdims=True)
        totals = jnp.sum(told, axis=0, keepdims=True)
        for t in range(count):
            peak = jnp.broadcast_to(peaks[:, t:t + 1], (8, LANES))
            gain = size / jnp.broadcast_to(totals[:, count + t:count + t + 1], (8, LANES))
            factor = peak * gain
            spread.append((gain, 0.002 * factor, 0.25 * factor))

    def tall(a):
        return jnp.concatenate([a] * (rows // 8), axis=0)

    def place(shift, k):
        return pl.multiple_of((lax.rem(chip + shift, chips) * chunks + k) * LANES, LANES)

    def columns(shift, k):
        return pl.ds(pl.multiple_of(core * starts[1] + place(shift, k), LANES), LANES)

    def pushed(shift):
        @on_each_core
        def _(c):
            for copy in push_copies(c, shift):
                copy.wait_recv()

    def partial(shift, k):
        here, full = pl.ds(place(shift, k), LANES), columns(shift, k)
        numer = denom = None
        for other in (0, 1):
            at = here if other else full
            for t in range(count):
                gain, low, high = (tall(a) for a in spread[other * count + t])
                info = (fisher_in if other else fisher)[t, :, at]
                theta = (params_in if other else params)[t, :, at].astype(f32)
                weight = jnp.minimum(jnp.maximum(info * gain, low), high)
                numer = weight * theta if numer is None else numer + weight * theta
                denom = weight if denom is None else denom + weight
        return numer, denom

    def y_copy(shift, k):
        return remote(sent.at[shift - 1, k], landed.at[shift - 1, k], y_send, y_recv.at[shift - 1, k],
                      device(shift, False, 0))

    def res_copy(shift, k):
        where = out.at[:, columns(0, k)]
        return remote(where, where, res_send, res_recv.at[shift - 1, k], device(shift, False, 0))

    def near_copy(shift, k):
        where = out.at[:, columns(chips - shift if shift else 0, k)]
        return remote(where, where, near_send, near_recv, partner)

    head = lax.broadcasted_iota(jnp.int32, (HEAD, LANES), 0)

    for shift in range(1, chips):
        pushed(shift)

        def send(k, carry, shift=shift):
            numer, denom = partial(shift, k)
            mean = numer / denom
            reach = jnp.maximum(jnp.max(jnp.abs(mean), axis=0, keepdims=True) * 1.01, 1e-35)
            reach = reach.astype(jnp.bfloat16).astype(f32)
            most = (jnp.max(denom, axis=0, keepdims=True) * 1.01).astype(jnp.bfloat16).astype(f32)
            box = sent.at[shift - 1, k]
            box[0:rows] = encode(mean * (1.0 / reach))
            box[rows:2 * rows] = encode(2.0 * jnp.sqrt(denom * (1.0 / most)) - 1.0)
            box[2 * rows:2 * rows + HEAD] = jnp.where(head == 0, reach, most).astype(jnp.bfloat16)
            y_copy(shift, k).start()
            return carry

        lax.fori_loop(0, chunks, send, 0)

    pushed(0)

    def keep(k, carry):
        kept[k, 0], kept[k, 1] = partial(0, k)
        return carry

    lax.fori_loop(0, chunks, keep, 0)

    def finish(k, carry):
        numer, denom = kept[k, 0], kept[k, 1]
        for shift in range(1, chips):
            y_copy(shift, k).wait_recv()
            box = landed.at[shift - 1, k]
            scale = box[2 * rows:2 * rows + HEAD].astype(f32)
            root = decode(box[rows:2 * rows]) * 0.5 + 0.5
            weight = root * root * scale[1:2]
            numer = numer + decode(box[0:rows]) * scale[0:1] * weight
            denom = denom + weight
        out[:, columns(0, k)] = (numer / denom).astype(out.dtype)
        for shift in range(1, chips):
            res_copy(shift, k).start()
        near_copy(0, k).start()
        return carry

    lax.fori_loop(0, chunks, finish, 0)

    for shift in range(1, chips):
        def forward(k, carry, shift=shift):
            res_copy(shift, k).wait_recv()
            near_copy(shift, k).start()
            return carry

        lax.fori_loop(0, chunks, forward, 0)

    stat_all.wait_send()

    @on_each_core
    def _(c):
        def strip(ref, size):
            return ref.at[:, pl.ds(0, size * LANES)]

        def whole(src, send):
            return remote(src, src, send, near_recv, partner)

        given = pl.ds(0, chips * counts[1 - c] * LANES)
        whole(fisher_hbm.at[:, :, given], push_f).wait_send()
        whole(params_hbm.at[:, :, given], push_p).wait_send()
        whole(sent.at[:, pl.ds(0, counts[c])], y_send).wait_send()
        whole(strip(out, (chips - 1) * counts[c]), res_send).wait_send()
        whole(strip(out, chips * counts[c]), near_send).wait_send()
        whole(strip(out, chips * counts[1 - c]), near_send).wait_recv()


def local(mesh, params, fisher):
    count, rows, width = fisher.shape
    tasks, groups = mesh.shape["task"], mesh.shape["param"]
    chips, chunks = tasks // 2, width // tasks // LANES
    counts = (chunks - chunks // 8, chunks + chunks // 8)
    most, far = counts[1], max(1, chips - 1)
    side = most * chips * LANES
    f32, bf16, dma = jnp.float32, jnp.bfloat16, pltpu.SemaphoreType.DMA
    return pl.pallas_call(
        functools.partial(kernel, tasks, groups, counts),
        out_shape=pltpu.VMEM((rows, width), bf16),
        in_specs=[pl.BlockSpec(memory_space=pltpu.HBM)] * 2,
        out_specs=pl.BlockSpec(memory_space=pltpu.VMEM),
        scratch_shapes=[
            pltpu.VMEM((count, rows, width), f32),
            pltpu.VMEM((count, rows, width), bf16),
            pltpu.VMEM((count, rows, side), f32),
            pltpu.VMEM((count, rows, side), bf16),
            pltpu.VMEM((8, LANES), f32),
            pltpu.VMEM((2 * groups, LANES), f32),
            pltpu.VMEM((far, most, 2 * rows + HEAD, LANES), bf16),
            pltpu.VMEM((far, most, 2 * rows + HEAD, LANES), bf16),
            pltpu.VMEM((most, 2, rows, LANES), f32),
            dma((count, 2)),
            dma(()),
            dma(()),
            dma(()),
            dma((chips,)),
            dma((chips,)),
            dma(()),
            dma(()),
            dma(()),
            dma((far, most)),
            dma(()),
            dma((far, most)),
            dma(()),
            dma(()),
        ],
        compiler_params=pltpu.CompilerParams(collective_id=0, has_side_effects=True),
        name="merge",
    )(params, fisher)


def solution(mesh):
    in_specs = (P("task", "param", None), P("task", "param", None))
    out_specs = P("param", None)
    return jax.shard_map(
        functools.partial(local, mesh), mesh=mesh, in_specs=in_specs, out_specs=out_specs, check_vma=False)
```
